256 devices in a mesh: unit: 4 (over y_lo, core), ep: 4 (over z_lo), fsdp: 16 (over z_hi, y_hi, x).
Axes of the slice: x: 4, y: 4 (y_hi: 2, y_lo: 2; y = y_hi * 2 + y_lo), z: 8 (z_hi: 2, z_lo: 4; z = z_hi * 4 + z_lo), core: 2. Of those that a mesh axis runs over, the one named last changes fastest.
Arguments:
- w_down: float32 [256, 1024, 2048], P(('unit', 'ep'), None, 'fsdp'), parts along dimension 0, may hold values from -0.25 to 0.25
- router_weight: float32 [8192, 64], P(('unit', 'fsdp'), 'ep'), parts along dimension 0, may hold values from -0.125 to 0.125
- router_gain: float32 [8192], P(('unit', 'fsdp')), parts along dimension 0, may hold values from 0.25 to 1.75
Outputs:
- serve_down: bfloat16 [256, 1024, 2048], P(('unit', 'ep'), 'fsdp'), parts along dimension 0
- scale_down: float32 [256, 1024], P(('unit', 'ep'), 'fsdp'), parts along dimension 0
- serve_router: bfloat16 [8192, 64], P('unit'), parts along dimension 0
The draws below stay inside these ranges and needn't reach their ends.
There are 4 independent parts, one for each index of `unit`. The reference program is written for one: setup_inputs(seed, part) draws one part's arguments, and reference() takes and returns one part's arrays. A program takes and returns all parts, laid end to end along the dimension named above; each array names one. Nothing has to cross between parts.
All inputs are finite; a program needn't handle non-finite values. Where the reference program divides by a largest or mean magnitude, that divisor is 1e-20 or more.
Results may differ from the reference program's by a relative error of at most 0.001.
Values may be sent and summed in bfloat16 or wider, within the bound.
No kernel may reach another device: no remote copies, remote signals or barrier semaphores. Data moves between devices by JAX's collectives and lax.ppermute only.
A program may use at most 64 MiB of HBM per device.

```python
import jax
import jax.numpy as jnp

EXPERTS = 64
D_MODEL = 2048
D_EXPERT = 1024


def spiked(entries, rng, source, target, blocks, factor):
    def block_of(dim):
        return (jnp.arange(entries.shape[dim]) // (entries.shape[dim] // blocks)).reshape((-1,) + (1,) * (entries.ndim - 1 - dim))

    first = jax.random.permutation(rng, blocks)[block_of(target)]
    far = (block_of(target) + blocks // 2) % blocks
    return jnp.where((block_of(source) == first) | (block_of(source) == far), factor * entries, entries)


def block_levels(stream_key, shape, split, least, high):
    level, own = 1.0, jax.random.fold_in(stream_key, 6)
    for axis_at, blocks in split:
        draws = jnp.exp(jax.random.uniform(jax.random.fold_in(own, axis_at), (blocks,), jnp.float32, least / len(split), high / len(split)))
        level = level * jnp.repeat(draws, shape[axis_at] // blocks).reshape([-1 if axis == axis_at else 1 for axis in range(len(shape))])
    return level


def bell_draw(rng, extent, width, most, pieces=(), held_as=jnp.bfloat16):
    loudness = block_levels(rng, extent, pieces, -0.22, 0.18) if pieces else 1.0
    drawn = jax.random.normal(rng, extent, jnp.float32) * width * loudness
    return jnp.minimum(jnp.maximum(drawn, -most), most).astype(held_as)


def bell_draw_with(rng, extent, scale, limit, pieces, heavy, kind=jnp.bfloat16):
    entries = scale * jax.random.normal(rng, extent, jnp.float32)
    if pieces:
        entries = entries * block_levels(rng, extent, pieces, -0.22, 0.18)
    return jnp.clip(spiked(entries, jax.random.fold_in(rng, 3), *heavy), -limit, limit).astype(kind)


def setup_inputs(seed: int = 0, part: int = 0) -> dict:
    splits = jax.random.split(jax.random.key(seed), 4)
    part_keys = jax.random.split(jax.random.fold_in(splits[3], part), 4)
    w_down = bell_draw_with(part_keys[0], (EXPERTS, D_EXPERT, D_MODEL), D_EXPERT ** -0.5, 0.25, ((0, 4), (2, 16)), (2, 1, 16, 2.0), jnp.float32)
    router_weight = bell_draw(part_keys[1], (D_MODEL, EXPERTS), D_MODEL ** -0.5, 0.125, ((0, 16), (1, 4)), jnp.float32)
    router_gain = jnp.clip(1.0 + 0.15 * jax.random.normal(part_keys[2], (D_MODEL,), jnp.float32), 0.25, 1.75)
    return {"w_down": w_down, "router_weight": router_weight, "router_gain": router_gain}


def reference(w_down, router_weight, router_gain):
    scale_down = jnp.sum(jnp.abs(w_down), axis=2) / D_MODEL
    serve_down = (w_down / jnp.expand_dims(scale_down, 2)).astype(jnp.bfloat16)
    serve_router = (router_weight * router_gain[:, None]).astype(jnp.bfloat16)
    return serve_down, scale_down, serve_router
```

```python
import functools

import jax
import jax.numpy as jnp
from jax import lax
from jax.experimental import pallas as pl
from jax.experimental.pallas import tpu as pltpu
from jax.sharding import PartitionSpec as P

D_MODEL = 2048
ROWS = 64
LANES = 128
GROUP = 16

E1, E2, F, L1, L2 = 2, 1, 5, 4, 4
E = E1 + E2


def swap(shard, k, axis="fsdp"):
    return lax.ppermute(shard, axis, [(i, i ^ k) for i in range(lax.axis_size(axis))])


def row_sums_kernel(w_ref, s_ref):
    rows = []
    for j in range(8):
        block = jnp.abs(w_ref[0, j * LANES : (j + 1) * LANES, :])
        rows.append(jnp.sum(block.T, axis=0, keepdims=True))
    s_ref[0] = jnp.concatenate(rows, axis=0)


def row_sums(w, first, count):
    return pl.pallas_call(
        row_sums_kernel,
        grid=(count,),
        in_specs=[pl.BlockSpec((1, 1024, LANES), lambda e: (e + first, 0, 0))],
        out_specs=pl.BlockSpec((1, 8, LANES), lambda e: (e, 0, 0)),
        out_shape=jax.ShapeDtypeStruct((count, 8, LANES), jnp.float32),
        name="row_sums",
        cost_estimate=pl.CostEstimate(
            flops=count * 250_000_0, bytes_accessed=count * 524_288, transcendentals=0
        ),
    )(w)


def relative(s, me):
    s = jnp.where((me & 8) != 0, jnp.concatenate([s[4:8], s[0:4]], 0), s)
    s = jnp.where((me & 4) != 0, jnp.concatenate([s[2:4], s[0:2], s[6:8], s[4:6]], 0), s)
    odd = [s[i ^ 1 : (i ^ 1) + 1] for i in range(8)]
    s = jnp.where((me & 2) != 0, jnp.concatenate(odd, 0), s)
    return jnp.where((me & 1) != 0, jnp.concatenate([s[:, ROWS:], s[:, :ROWS]], 1), s)


def spread_kernel(places, scaled, me_ref, *refs):
    me = me_ref[0]
    w_ref = refs[0]
    outs = refs[2:] if scaled else refs[1:]
    if scaled:
        t = (D_MODEL / relative(refs[1][0], me)).T
    for r in range(GROUP):
        block = w_ref[0, pl.ds(pl.multiple_of((me ^ r) * ROWS, ROWS), ROWS), :]
        if scaled:
            h = (r & 1) * ROWS
            block = block * t[h : h + ROWS, r >> 1 : (r >> 1) + 1]
        array, place = places[r]
        outs[array][place, 0] = block.astype(outs[array].dtype)


def spread(w, sums, me, first, count, places, sizes, skip=0):
    scaled = sums is not None
    kind = jnp.bfloat16 if scaled else jnp.float32
    in_specs = [pl.BlockSpec((1, 1024, LANES), lambda e, m: (e + first, 0, 0))]
    args = [w]
    if scaled:
        in_specs.append(pl.BlockSpec((1, 8, LANES), lambda e, m: (e + skip, 0, 0)))
        args.append(sums)
    return pl.pallas_call(
        functools.partial(spread_kernel, places, scaled),
        grid_spec=pltpu.PrefetchScalarGridSpec(
            num_scalar_prefetch=1,
            grid=(count,),
            in_specs=in_specs,
            out_specs=[
                pl.BlockSpec((n, 1, ROWS, LANES), lambda e, m: (0, e, 0, 0)) for n in sizes
            ],
        ),
        out_shape=[jax.ShapeDtypeStruct((n, count, ROWS, LANES), kind) for n in sizes],
        name="spread",
        cost_estimate=pl.CostEstimate(
            flops=count * 250_000_0, bytes_accessed=count * 786_432, transcendentals=0
        ),
    )(me, *args)


def join_kernel(pieces, raw, count, me_ref, *refs):
    me = me_ref[0]
    ins = refs[: len(pieces)]
    out_ref = refs[len(pieces) + (0 if raw else 1)]
    blocks = {}
    for ref, where in zip(ins, pieces, strict=True):
        for place, r in where:
            blocks[r] = (ref, place)
    inverse = None
    if raw:
        total = None
        for r in range(GROUP):
            ref, place = blocks[r]
            part = jnp.abs(ref[place, 0])
            total = part if total is None else total + part
        total = jnp.sum(total, axis=1, keepdims=True)
        scale = jnp.broadcast_to(total / D_MODEL, (ROWS, LANES))
        refs[-1][0] = scale.T[0:8]
        inverse = 1.0 / scale
    for r in range(GROUP):
        ref, place = blocks[r]
        block = ref[place, 0]
        if raw:
            block = (block * inverse).astype(jnp.bfloat16)
        out_ref[0, :, pl.ds(pl.multiple_of((me ^ r) * LANES, LANES), LANES)] = block


def join(out, pieces, me, first, count, raw=False):
    in_specs, args, where = [], [], []
    for array, start, taken, rs in pieces:
        assert start % taken == 0
        in_specs.append(
            pl.BlockSpec(
                (taken, 1, ROWS, LANES),
                functools.partial(lambda at, e, m: (at, e, 0, 0), start // taken),
            )
        )
        args.append(array)
        where.append([(i, r) for i, r in enumerate(rs)])
    out_shape = [jax.ShapeDtypeStruct((GROUP, ROWS, D_MODEL), jnp.bfloat16)]
    out_specs = [pl.BlockSpec((1, ROWS, D_MODEL), lambda e, m: (e + first, 0, 0))]
    alias = {}
    if raw:
        out_shape.append(jax.ShapeDtypeStruct((count, 8, ROWS), jnp.float32))
        out_specs.append(pl.BlockSpec((1, 8, ROWS), lambda e, m: (e, 0, 0)))
    else:
        in_specs.append(pl.BlockSpec(memory_space=pl.ANY))
        args.append(out)
        alias = {len(args): 0}
    return pl.pallas_call(
        functools.partial(join_kernel, where, raw, count),
        grid_spec=pltpu.PrefetchScalarGridSpec(
            num_scalar_prefetch=1, grid=(count,), in_specs=in_specs, out_specs=out_specs
        ),
        out_shape=out_shape,
        input_output_aliases=alias,
        name="join",
        cost_estimate=pl.CostEstimate(
            flops=count * 250_000_0, bytes_accessed=count * 524_288, transcendentals=0
        ),
    )(me, *args)


def r_of(z, y, x):
    return z * 8 + y * 4 + x


Z_FIRST = [(r >> 3, r & 7) for r in range(GROUP)]
X_FIRST = [(r & 3, ((r >> 2) & 1) * 2 + (r >> 3)) for r in range(GROUP)]


def finish_z_first(kept, came):
    over_y = swap(jnp.concatenate([kept[4:8], came[4:8]], 0), 4)
    pieces = [
        (kept, 0, 1, [r_of(0, 0, 0)]),
        (came, 0, 1, [r_of(1, 0, 0)]),
        (over_y, 0, 1, [r_of(0, 1, 0)]),
        (over_y, 4, 1, [r_of(1, 1, 0)]),
    ]
    for k in (1, 2, 3):
        sent = [kept[k : k + 1], came[k : k + 1], over_y[k : k + 1], over_y[4 + k : 5 + k]]
        over_x = swap(jnp.concatenate(sent, 0), k)
        pieces.append((over_x, 0, 4, [r_of(0, 0, k), r_of(1, 0, k), r_of(0, 1, k), r_of(1, 1, k)]))
    return pieces


def start_x_first(arrays):
    have = [arrays[0]] + [swap(arrays[k], k) for k in (1, 2, 3)]
    over_y = swap(jnp.concatenate([a[2:4] for a in have], 0), 4)
    sent = [a[1:2] for a in have] + [over_y[2 * x + 1 : 2 * x + 2] for x in range(4)]
    return have, over_y, jnp.concatenate(sent, 0)


def finish_x_first(have, over_y, came):
    pieces = [(have[x], 0, 1, [r_of(0, 0, x)]) for x in range(4)]
    pieces += [(over_y, 2 * x, 1, [r_of(0, 1, x)]) for x in range(4)]
    pieces.append((came, 0, 8, [r_of(1, y, x) for y in range(2) for x in range(4)]))
    return pieces


def copy_for_each(shard, axis):
    length = lax.axis_size(axis)
    return lax.all_to_all(
        jnp.broadcast_to(shard[None], (length, *shard.shape)), axis, 0, 0, tiled=True
    )


def laid_out(tiles, dim):
    tiles = jnp.moveaxis(tiles, 0, dim)
    lengths = tiles.shape
    return tiles.reshape(*lengths[:dim], lengths[dim] * lengths[dim + 1], *lengths[dim + 2 :])


def gathered_copies(shard, axis, dim):
    return laid_out(copy_for_each(shard, axis), dim)


def on_device(w_down, router_weight, router_gain):
    index = lax.axis_index("fsdp")
    me = index.astype(jnp.int32).reshape(1)

    kept1, sent1 = spread(w_down, None, me, 0, E1, Z_FIRST, (8, 8))
    kept2, sent2 = spread(w_down, None, me, E1, E2, Z_FIRST, (8, 8))
    came1 = swap(sent1, 8)

    sums = row_sums(w_down, E, GROUP - E)
    for k in (1, 2, 4):
        sums = sums + swap(sums, k)
    came_sums = swap(sums, 8)
    came2 = swap(sent2, 8)
    sums = sums + came_sums

    kept_f, sent_f = spread(w_down, sums, me, E, F, Z_FIRST, (8, 8), 0)
    came_f = swap(sent_f, 8)
    at1 = E + F
    first = spread(w_down, sums, me, at1, L1, X_FIRST, (4,) * 4, F)
    have1, over1, last1 = start_x_first(first)
    came_l1 = swap(last1, 8)
    second = spread(w_down, sums, me, at1 + L1, L2, X_FIRST, (4,) * 4, F + L1)
    have2, over2, last2 = start_x_first(second)
    came_l2 = swap(last2, 8)

    kept = jnp.concatenate([kept1, kept2], 1)
    came = jnp.concatenate([came1, came2], 1)
    out, scale_e = join(None, finish_z_first(kept, came), me, 0, E, raw=True)
    (out,) = join(out, finish_z_first(kept_f, came_f), me, E, F)
    (out,) = join(out, finish_x_first(have1, over1, came_l1), me, at1, L1)
    (out,) = join(out, finish_x_first(have2, over2, came_l2), me, at1 + L1, L2)

    own = lax.dynamic_slice_in_dim(sums.reshape(GROUP - E, GROUP, ROWS), index, 1, 1)[:, 0]
    scale_down = jnp.concatenate([scale_e[:, 0], own / D_MODEL], 0)

    part_router = (router_weight * router_gain[:, None]).astype(jnp.bfloat16)
    row_router = gathered_copies(part_router, "fsdp", 0)
    serve_router = gathered_copies(row_router, "ep", 1)
    return (out, scale_down, serve_router)


def solution(mesh):
    return jax.shard_map(
        on_device,
        mesh=mesh,
        in_specs=(P(("unit", "ep"), None, "fsdp"), P(("unit", "fsdp"), "ep"), P(("unit", "fsdp"))),
        out_specs=(P(("unit", "ep"), "fsdp", None), P(("unit", "ep"), "fsdp"), P("unit", None)),
        check_vma=False,
    )
```

```python
import functools

import jax
import jax.numpy as jnp
from jax import lax
from jax.experimental import pallas as pl
from jax.experimental.pallas import tpu as pltpu
from jax.sharding import PartitionSpec as P

D_MODEL = 2048
EXPERTS = 16
ROWS = 64
LANES = 128
HALF = 512
PLANES = [list(range(8)), list(range(8, 16))]

E, F1, F2, L = (0, 2), (2, 6), (8, 4), (12, 4)
OWN = (2, 14)


def swap(shard, k, axis="fsdp"):
    return lax.ppermute(shard, axis, [(i, i ^ k) for i in range(lax.axis_size(axis))])


def in_plane(shard):
    return lax.all_to_all(shard, "fsdp", 0, 0, axis_index_groups=PLANES, tiled=True)


def tie(value, *others):
    return lax.optimization_barrier((value, *others))[0]


def spread_kernel(other, scaled, z_ref, w_ref, *refs):
    out_ref = refs[-1]
    high = (z_ref[0] ^ other) == 1
    for i in range(w_ref.shape[0]):
        if scaled:
            tile = refs[0][i]
            tile = jnp.where(high, jnp.concatenate([tile[4:8], tile[0:4]], 0), tile)
            inverse = (D_MODEL / tile).T
        for j in range(4):
            block = w_ref[i, j * LANES : (j + 1) * LANES, :]
            if scaled:
                block = block * inverse[:, j : j + 1]
            block = block.astype(out_ref.dtype)
            out_ref[2 * j, i] = block[:ROWS]
            out_ref[2 * j + 1, i] = block[ROWS:]


def spread(w, sums, z, which, other, step):
    first, count = which
    scaled = sums is not None
    kind = jnp.bfloat16 if scaled else jnp.float32
    assert first % step == 0 and count % step == 0
    at = first // step
    in_specs = [pl.BlockSpec((step, HALF, LANES), lambda e, z: (at + e, z[0] ^ other, 0))]
    args = [w]
    if scaled:
        in_specs.append(pl.BlockSpec((step, 8, LANES), lambda e, z: (at + e, 0, 0)))
        args.append(sums)
    return pl.pallas_call(
        functools.partial(spread_kernel, other, scaled),
        grid_spec=pltpu.PrefetchScalarGridSpec(
            num_scalar_prefetch=1,
            grid=(count // step,),
            in_specs=in_specs,
            out_specs=pl.BlockSpec((8, step, ROWS, LANES), lambda e, z: (0, e, 0, 0)),
        ),
        out_shape=jax.ShapeDtypeStruct((8, count, ROWS, LANES), kind),
        name="spread",
        cost_estimate=pl.CostEstimate(
            flops=count * 1_000_000, bytes_accessed=count * 393_216, transcendentals=0
        ),
    )(z, *args)


def join_kernel(scaled, z_ref, in_ref, *refs):
    out_ref = refs[-1]
    for i in range(out_ref.shape[0]):
        for g in range(8):
            block = in_ref[g, i]
            if scaled:
                block = block * refs[0][i]
            out_ref[i, :, g * LANES : (g + 1) * LANES] = block.astype(jnp.bfloat16)


def join(out, came, inverse, z, which, other, step):
    first, count = which
    assert first % step == 0 and count % step == 0
    at = first // step
    in_specs = [pl.BlockSpec((8, step, ROWS, LANES), lambda e, z: (0, e, 0, 0))]
    args = [came]
    if inverse is not None:
        in_specs.append(pl.BlockSpec((step, ROWS, LANES), lambda e, z: (e, 0, 0)))
        args.append(inverse)
    alias = {}
    if out is not None:
        in_specs.append(pl.BlockSpec(memory_space=pl.ANY))
        args.append(out)
        alias = {len(args): 0}
    return pl.pallas_call(
        functools.partial(join_kernel, inverse is not None),
        grid_spec=pltpu.PrefetchScalarGridSpec(
            num_scalar_prefetch=1,
            grid=(count // step,),
            in_specs=in_specs,
            out_specs=pl.BlockSpec((step, ROWS, 1024), lambda e, z: (at + e, 0, z[0] ^ other)),
        ),
        out_shape=jax.ShapeDtypeStruct((EXPERTS, ROWS, D_MODEL), jnp.bfloat16),
        input_output_aliases=alias,
        name="join",
        cost_estimate=pl.CostEstimate(
            flops=count * 1_000_000, bytes_accessed=count * 262_144, transcendentals=0
        ),
    )(z, *args)


def on_device(w_down, router_weight, router_gain):
    index = lax.axis_index("fsdp").astype(jnp.int32)
    z = (index // 8).reshape(1)

    raw = spread(w_down, None, z, E, 1, 2)
    came_e = swap(raw, 8)
    own_e = spread(w_down, None, z, E, 0, 2)
    sums = jnp.sum(jnp.abs(w_down), axis=2).reshape(EXPERTS, 8, LANES)
    for k in (1, 2, 4):
        sums = sums + swap(sums, k)
    came = swap(sums, 8)

    part = (router_weight * router_gain[:, None]).astype(jnp.bfloat16).T
    part = tie(part, sums)
    part = lax.all_to_all(jnp.broadcast_to(part[None], (4, 16, LANES)), "ep", 0, 0, tiled=True)
    part = part.reshape(ROWS, LANES)
    sums = sums + came

    oth_f1 = spread(w_down, sums, z, F1, 1, 2)
    came_f1 = swap(oth_f1, 8)
    oth_l = spread(w_down, sums, z, L, 1, 2)
    oth_f2 = spread(w_down, sums, z, F2, 1, 2)
    came_f2 = swap(oth_f2, 8)
    plane_l = in_plane(oth_l)
    own = spread(w_down, sums, z, OWN, 0, 2)
    other_part = swap(part, 8)
    came_l = swap(plane_l, 8)
    own = in_plane(own)
    own_e = in_plane(tie(own_e, oth_f2))
    came_e = in_plane(came_e)

    scale = lax.dynamic_slice_in_dim(sums.reshape(EXPERTS, 16, ROWS), index, 1, 1)[:, 0] / D_MODEL
    inverse = jnp.broadcast_to((1.0 / scale[:2])[:, :, None], (2, ROWS, LANES))

    came_f1 = in_plane(came_f1)
    both = jnp.broadcast_to(jnp.stack([part, other_part])[None], (8, 2, ROWS, LANES))
    both = in_plane(both)
    came_f2 = in_plane(came_f2)

    out = join(None, own_e, inverse, z, E, 0, 2)
    out = join(out, own, None, z, OWN, 0, 2)
    out = join(out, came_e, inverse, z, E, 1, 2)
    out = join(out, came_f1, None, z, F1, 1, 2)
    out = join(out, came_f2, None, z, F2, 1, 4)
    out = join(out, came_l, None, z, L, 1, 4)

    halves = both.transpose(1, 2, 0, 3).reshape(2, ROWS, 1024)
    halves = jnp.where(z[0] == 0, halves, halves[::-1])
    router = jnp.concatenate([halves[0], halves[1]], 1).T
    return (out, scale, router)


def solution(mesh):
    return jax.shard_map(
        on_device,
        mesh=mesh,
        in_specs=(P(("unit", "ep"), None, "fsdp"), P(("unit", "fsdp"), "ep"), P(("unit", "fsdp"))),
        out_specs=(P(("unit", "ep"), "fsdp", None), P(("unit", "ep"), "fsdp"), P("unit", None)),
        check_vma=False,
    )
```

```python
import functools

import jax
import jax.numpy as jnp
from jax import lax
from jax.experimental import pallas as pl
from jax.experimental.pallas import tpu as pltpu
from jax.sharding import PartitionSpec as P

D_MODEL = 2048
EXPERTS = 16
ROWS = 64
LANES = 128
HALF = 512

F, L, E = (0, 7), (7, 7), (14, 2)
A, B = (0, 10), (10, 6)


def swap(shard, k):
    return lax.ppermute(shard, "fsdp", [(i, i ^ k) for i in range(lax.axis_size("fsdp"))])


def relative(s, m):
    s = jnp.where((m & 8) != 0, jnp.concatenate([s[4:8], s[0:4]], 0), s)
    s = jnp.where((m & 4) != 0, jnp.concatenate([s[2:4], s[0:2], s[6:8], s[4:6]], 0), s)
    odd = [s[i ^ 1 : (i ^ 1) + 1] for i in range(8)]
    s = jnp.where((m & 2) != 0, jnp.concatenate(odd, 0), s)
    return jnp.where((m & 1) != 0, jnp.concatenate([s[:, ROWS:], s[:, :ROWS]], 1), s)


def spread_kernel(other, scaled, me_ref, w_ref, *refs):
    m = me_ref[0] ^ (8 * other)
    outs = refs[1:] if scaled else refs
    for i in range(w_ref.shape[0]):
        if scaled:
            inverse = (D_MODEL / relative(refs[0][i], m)).T
        for r in range(8):
            at = pl.multiple_of(((m & 7) ^ r) * ROWS, ROWS)
            block = w_ref[i, pl.ds(at, ROWS), :]
            if scaled:
                h = (r & 1) * ROWS
                block = block * inverse[h : h + ROWS, r >> 1 : (r >> 1) + 1]
            y, x = r >> 2, r & 3
            if len(outs) == w_ref.shape[0] and not scaled:
                outs[i][2 * x + y, 0] = block.astype(outs[i].dtype)
            elif len(outs) == 4:
                outs[x][y, i] = block.astype(outs[x].dtype)
            else:
                outs[0][2 * x + y, i] = block.astype(outs[0].dtype)


def spread(w, sums, me, which, other, arrays, step):
    first, count = which
    scaled = sums is not None
    kind = jnp.bfloat16 if scaled else jnp.float32
    assert count % step == 0
    blocks = 8 // arrays
    in_specs = [
        pl.BlockSpec(
            (pl.Element(step), pl.Element(HALF), pl.Element(LANES)),
            lambda e, m: (first + e * step, ((m[0] >> 3) ^ other) * HALF, 0),
        )
    ]
    args = [w]
    if scaled:
        in_specs.append(
            pl.BlockSpec(
                (pl.Element(step), pl.Element(8), pl.Element(LANES)),
                lambda e, m: (first + e * step, 0, 0),
            )
        )
        args.append(sums)
    return pl.pallas_call(
        functools.partial(spread_kernel, other, scaled),
        grid_spec=pltpu.PrefetchScalarGridSpec(
            num_scalar_prefetch=1,
            grid=(count // step,),
            in_specs=in_specs,
            out_specs=[pl.BlockSpec((blocks, step, ROWS, LANES), lambda e, m: (0, e, 0, 0))]
            * arrays,
        ),
        out_shape=[jax.ShapeDtypeStruct((blocks, count, ROWS, LANES), kind)] * arrays,
        name="spread",
        cost_estimate=pl.CostEstimate(
            flops=count * 1_000_000, bytes_accessed=count * 393_216, transcendentals=0
        ),
    )(me, *args)


def own_kernel(me_ref, w_ref, s_ref, router_ref, *refs):
    m = me_ref[0]
    raws, outs = refs[:-2], refs[-2:]
    count = w_ref.shape[0]
    for i in range(count):
        inverse = (D_MODEL / relative(s_ref[i], m)).T
        for r in range(8):
            at = pl.multiple_of(((m & 7) ^ r) * ROWS, ROWS)
            column = inverse[(r & 1) * ROWS : (r & 1) * ROWS + ROWS, r >> 1 : (r >> 1) + 1]
            outs[r >> 2][r & 3, i] = (w_ref[i, pl.ds(at, ROWS), :] * column).astype(jnp.bfloat16)
            raw = i - (count - len(raws))
            if raw >= 0:
                block = raws[raw][2 * (r & 3) + (r >> 2), 0] * column
                outs[r >> 2][r & 3, count + 2 + raw] = block.astype(jnp.bfloat16)
    for out in outs:
        for x in range(4):
            for z in range(2):
                out[x, count + z] = router_ref[z]


def spread_own(w, sums, router, raws, me, which):
    first, count = which
    slots = count + 2 + len(raws)

    def whole(*shape):
        return pl.BlockSpec(shape, lambda e, m: (0,) * len(shape))

    return pl.pallas_call(
        own_kernel,
        grid_spec=pltpu.PrefetchScalarGridSpec(
            num_scalar_prefetch=1,
            grid=(1,),
            in_specs=[
                pl.BlockSpec(
                    (pl.Element(count), pl.Element(HALF), pl.Element(LANES)),
                    lambda e, m: (first, (m[0] >> 3) * HALF, 0),
                ),
                pl.BlockSpec(
                    (pl.Element(count), pl.Element(8), pl.Element(LANES)),
                    lambda e, m: (first, 0, 0),
                ),
                whole(2, ROWS, LANES),
            ]
            + [whole(8, 1, ROWS, LANES)] * len(raws),
            out_specs=[whole(4, slots, ROWS, LANES)] * 2,
        ),
        out_shape=[jax.ShapeDtypeStruct((4, slots, ROWS, LANES), jnp.bfloat16)] * 2,
        name="spread_own",
        cost_estimate=pl.CostEstimate(
            flops=slots * 1_000_000, bytes_accessed=slots * 393_216, transcendentals=0
        ),
    )(me, w, sums, router, *raws)


def spread_raw(w, me, which):
    first, count = which
    return pl.pallas_call(
        functools.partial(spread_kernel, 1, False),
        grid_spec=pltpu.PrefetchScalarGridSpec(
            num_scalar_prefetch=1,
            grid=(1,),
            in_specs=[
                pl.BlockSpec(
                    (pl.Element(count), pl.Element(HALF), pl.Element(LANES)),
                    lambda e, m: (first, ((m[0] >> 3) ^ 1) * HALF, 0),
                )
            ],
            out_specs=[pl.BlockSpec((8, 1, ROWS, LANES), lambda e, m: (0, 0, 0, 0))] * count,
        ),
        out_shape=[jax.ShapeDtypeStruct((8, 1, ROWS, LANES), jnp.float32)] * count,
        name="spread_raw",
        cost_estimate=pl.CostEstimate(
            flops=count * 1_000_000, bytes_accessed=count * 524_288, transcendentals=0
        ),
    )(me, w)


def join_kernel(where, me_ref, *refs):
    me = me_ref[0]
    out_ref = refs[-1]
    for i in range(out_ref.shape[0]):
        for ref, places in zip(refs, where):
            for place, r in places:
                at = pl.multiple_of(((me & 7) ^ r) * LANES, LANES)
                out_ref[i, :, pl.ds(at, LANES)] = ref[place, i]


def join(out, pieces, me, which, other, step, slot=0):
    first, count = which
    assert count % step == 0 and slot % step == 0
    base = slot // step
    in_specs, args, where = [], [], []
    for array, taken, rs in pieces:
        in_specs.append(pl.BlockSpec((taken, step, ROWS, LANES), lambda e, m: (0, base + e, 0, 0)))
        args.append(array)
        where.append([(i, r) for i, r in enumerate(rs)])
    alias = {}
    if out is not None:
        in_specs.append(pl.BlockSpec(memory_space=pl.ANY))
        args.append(out)
        alias = {len(args): 0}
    return pl.pallas_call(
        functools.partial(join_kernel, where),
        grid_spec=pltpu.PrefetchScalarGridSpec(
            num_scalar_prefetch=1,
            grid=(count // step,),
            in_specs=in_specs,
            out_specs=pl.BlockSpec(
                (pl.Element(step), pl.Element(ROWS), pl.Element(1024)),
                lambda e, m: (first + e * step, 0, ((m[0] >> 3) ^ other) * 1024),
            ),
        ),
        out_shape=jax.ShapeDtypeStruct((EXPERTS, ROWS, D_MODEL), jnp.bfloat16),
        input_output_aliases=alias,
        name="join",
        cost_estimate=pl.CostEstimate(
            flops=count * 1_000_000, bytes_accessed=count * 262_144, transcendentals=0
        ),
    )(me, *args)


def plane(arrays):
    have = [arrays[0]] + [swap(arrays[k], k) for k in (1, 2, 3)]
    over_y = swap(jnp.concatenate([a[1:2] for a in have], 0), 4)
    return have, over_y


def plane_y(arrays):
    kept, sent = arrays
    over_y = swap(sent, 4)
    pieces = [(kept, 1, [0]), (over_y, 1, [4])]
    for k in (1, 2, 3):
        both = jnp.concatenate([kept[k : k + 1], over_y[k : k + 1]], 0)
        pieces.append((swap(both, k), 2, [k, 4 + k]))
    return pieces


def by_x(came):
    return [came[2 * k : 2 * k + 2] for k in range(4)]


def pieces_of(have, over_y):
    return [(have[k], 1, [k]) for k in range(4)] + [(over_y, 4, [4, 5, 6, 7])]


def router_kernel(where, me_ref, *refs):
    me = me_ref[0]
    for ref, places in zip(refs, where):
        for place, r in places:
            for z in range(2):
                at = pl.multiple_of((me ^ (8 * z + r)) * LANES, LANES)
                refs[-1][:, pl.ds(at, LANES)] = ref[place, z]


def router_join(pieces, me, slot):
    where = [list(enumerate(rs)) for _, _, rs in pieces]
    assert slot % 2 == 0
    return pl.pallas_call(
        functools.partial(router_kernel, where),
        grid_spec=pltpu.PrefetchScalarGridSpec(
            num_scalar_prefetch=1,
            grid=(1,),
            in_specs=[
                pl.BlockSpec((taken, 2, ROWS, LANES), lambda e, m: (0, slot // 2, 0, 0))
                for _, taken, _ in pieces
            ],
            out_specs=pl.BlockSpec((ROWS, D_MODEL), lambda e, m: (0, 0)),
        ),
        out_shape=jax.ShapeDtypeStruct((ROWS, D_MODEL), jnp.bfloat16),
        name="router",
        cost_estimate=pl.CostEstimate(flops=2_000_000, bytes_accessed=524_288, transcendentals=0),
    )(me, *[array for array, _, _ in pieces])


def on_device(w_down, router_weight, router_gain):
    index = lax.axis_index("fsdp").astype(jnp.int32)
    me = index.reshape(1)

    sums = jnp.sum(jnp.abs(w_down), axis=2).reshape(EXPERTS, 8, LANES)
    for k in (1, 2, 4, 8):
        sums = sums + swap(sums, k)

    part = (router_weight * router_gain[:, None]).astype(jnp.bfloat16).T
    part = lax.all_to_all(jnp.broadcast_to(part[None], (4, 16, LANES)), "ep", 0, 0, tiled=True)
    part = part.reshape(ROWS, LANES)
    router = jnp.stack([part, swap(part, 8)])

    raws = spread_raw(w_down, me, E)
    raws = [swap(raw, 8) for raw in raws]

    (oth_f,) = spread(w_down, sums, me, F, 1, 1, 7)
    came_f = swap(oth_f, 8)
    oth_l = spread(w_down, sums, me, L, 1, 4, 7)
    own_b = spread_own(w_down, sums, router, raws, me, B)
    own_a = spread(w_down, sums, me, A, 0, 4, 5)

    plane_l = plane(oth_l)
    last = jnp.concatenate([a[0:1] for a in plane_l[0]] + [plane_l[1]], 0)
    came_l = swap(last, 8)
    plane_b = plane_y(own_b)
    plane_a = plane(own_a)
    plane_f = plane(by_x(came_f))

    scale = lax.dynamic_slice_in_dim(sums.reshape(EXPERTS, 16, ROWS), index, 1, 1)[:, 0] / D_MODEL

    out = join(None, pieces_of(*plane_a), me, A, 0, 5)
    out = join(out, plane_b, me, B, 0, B[1])
    serve_router = router_join(plane_b, me, B[1]).T
    out = join(out, plane_b, me, E, 1, 2, B[1] + 2)
    out = join(out, pieces_of(*plane_f), me, F, 1, 7)
    out = join(out, [(came_l, 8, list(range(8)))], me, L, 1, 7)
    return (out, scale, serve_router)


def solution(mesh):
    return jax.shard_map(
        on_device,
        mesh=mesh,
        in_specs=(P(("unit", "ep"), None, "fsdp"), P(("unit", "fsdp"), "ep"), P(("unit", "fsdp"))),
        out_specs=(P(("unit", "ep"), "fsdp", None), P(("unit", "ep"), "fsdp"), P("unit", None)),
        check_vma=False,
    )
```

```python
import functools

import jax
import jax.numpy as jnp
from jax import lax
from jax.experimental import pallas as pl
from jax.experimental.pallas import tpu as pltpu
from jax.sharding import PartitionSpec as P

D_MODEL = 2048
EXPERTS = 16
ROWS = 64
LANES = 128
HALF = 512

F, L, E = (0, 7), (7, 7), (14, 2)
A, B = (0, 10), (10, 6)


def swap(shard, k):
    return lax.ppermute(shard, "fsdp", [(i, i ^ k) for i in range(lax.axis_size("fsdp"))])


def pack(parts):
    return jnp.concatenate([array[first:end] for array, first, end in parts], 0)


def relative(s, m):
    s = jnp.where((m & 8) != 0, jnp.concatenate([s[4:8], s[0:4]], 0), s)
    s = jnp.where((m & 4) != 0, jnp.concatenate([s[2:4], s[0:2], s[6:8], s[4:6]], 0), s)
    odd = [s[i ^ 1 : (i ^ 1) + 1] for i in range(8)]
    s = jnp.where((m & 2) != 0, jnp.concatenate(odd, 0), s)
    return jnp.where((m & 1) != 0, jnp.concatenate([s[:, ROWS:], s[:, :ROWS]], 1), s)


def spread_kernel(other, scaled, me_ref, w_ref, *refs):
    m = me_ref[0] ^ (8 * other)
    outs = refs[1:] if scaled else refs
    for i in range(w_ref.shape[0]):
        if scaled:
            inverse = (D_MODEL / relative(refs[0][i], m)).T
        for r in range(8):
            at = pl.multiple_of(((m & 7) ^ r) * ROWS, ROWS)
            block = w_ref[i, pl.ds(at, ROWS), :]
            if scaled:
                h = (r & 1) * ROWS
                block = block * inverse[h : h + ROWS, r >> 1 : (r >> 1) + 1]
            y, x = r >> 2, r & 3
            if len(outs) == w_ref.shape[0] and not scaled:
                outs[i][2 * x + y, 0] = block.astype(outs[i].dtype)
            elif len(outs) == 4:
                outs[x][y, i] = block.astype(outs[x].dtype)
            else:
                outs[0][2 * x + y, i] = block.astype(outs[0].dtype)


def spread(w, sums, me, which, other, arrays, step):
    first, count = which
    scaled = sums is not None
    kind = jnp.bfloat16 if scaled else jnp.float32
    assert count % step == 0
    blocks = 8 // arrays
    in_specs = [
        pl.BlockSpec(
            (pl.Element(step), pl.Element(HALF), pl.Element(LANES)),
            lambda e, m: (first + e * step, ((m[0] >> 3) ^ other) * HALF, 0),
        )
    ]
    args = [w]
    if scaled:
        in_specs.append(
            pl.BlockSpec(
                (pl.Element(step), pl.Element(8), pl.Element(LANES)),
                lambda e, m: (first + e * step, 0, 0),
            )
        )
        args.append(sums)
    return pl.pallas_call(
        functools.partial(spread_kernel, other, scaled),
        grid_spec=pltpu.PrefetchScalarGridSpec(
            num_scalar_prefetch=1,
            grid=(count // step,),
            in_specs=in_specs,
            out_specs=[pl.BlockSpec((blocks, step, ROWS, LANES), lambda e, m: (0, e, 0, 0))]
            * arrays,
        ),
        out_shape=[jax.ShapeDtypeStruct((blocks, count, ROWS, LANES), kind)] * arrays,
        name="spread",
        cost_estimate=pl.CostEstimate(
            flops=count * 1_000_000, bytes_accessed=count * 393_216, transcendentals=0
        ),
    )(me, *args)


def own_kernel(me_ref, w_ref, s_ref, near_ref, far_ref, *refs):
    m = me_ref[0]
    raws, outs = refs[:-2], refs[-2:]
    count = w_ref.shape[0]
    for i in range(count):
        inverse = (D_MODEL / relative(s_ref[i], m)).T
        for r in range(8):
            at = pl.multiple_of(((m & 7) ^ r) * ROWS, ROWS)
            column = inverse[(r & 1) * ROWS : (r & 1) * ROWS + ROWS, r >> 1 : (r >> 1) + 1]
            outs[r >> 2][r & 3, i] = (w_ref[i, pl.ds(at, ROWS), :] * column).astype(jnp.bfloat16)
            raw = i - (count - len(raws))
            if raw >= 0:
                block = raws[raw][2 * (r & 3) + (r >> 2), 0] * column
                outs[r >> 2][r & 3, count + 2 + raw] = block.astype(jnp.bfloat16)
    for out in outs:
        for x in range(4):
            out[x, count] = near_ref[...]
            out[x, count + 1] = far_ref[...]


def spread_own(w, sums, router, raws, me, which):
    first, count = which
    slots = count + 2 + len(raws)

    def whole(*shape):
        return pl.BlockSpec(shape, lambda e, m: (0,) * len(shape))

    return pl.pallas_call(
        own_kernel,
        grid_spec=pltpu.PrefetchScalarGridSpec(
            num_scalar_prefetch=1,
            grid=(1,),
            in_specs=[
                pl.BlockSpec(
                    (pl.Element(count), pl.Element(HALF), pl.Element(LANES)),
                    lambda e, m: (first, (m[0] >> 3) * HALF, 0),
                ),
                pl.BlockSpec(
                    (pl.Element(count), pl.Element(8), pl.Element(LANES)),
                    lambda e, m: (first, 0, 0),
                ),
                whole(ROWS, LANES),
                whole(ROWS, LANES),
            ]
            + [whole(8, 1, ROWS, LANES)] * len(raws),
            out_specs=[whole(4, slots, ROWS, LANES)] * 2,
        ),
        out_shape=[jax.ShapeDtypeStruct((4, slots, ROWS, LANES), jnp.bfloat16)] * 2,
        name="spread_own",
        cost_estimate=pl.CostEstimate(
            flops=slots * 1_000_000, bytes_accessed=slots * 393_216, transcendentals=0
        ),
    )(me, w, sums, *router, *raws)


def spread_raw(w, me, which):
    first, count = which
    return pl.pallas_call(
        functools.partial(spread_kernel, 1, False),
        grid_spec=pltpu.PrefetchScalarGridSpec(
            num_scalar_prefetch=1,
            grid=(1,),
            in_specs=[
                pl.BlockSpec(
                    (pl.Element(count), pl.Element(HALF), pl.Element(LANES)),
                    lambda e, m: (first, ((m[0] >> 3) ^ 1) * HALF, 0),
                )
            ],
            out_specs=[pl.BlockSpec((8, 1, ROWS, LANES), lambda e, m: (0, 0, 0, 0))] * count,
        ),
        out_shape=[jax.ShapeDtypeStruct((8, 1, ROWS, LANES), jnp.float32)] * count,
        name="spread_raw",
        cost_estimate=pl.CostEstimate(
            flops=count * 1_000_000, bytes_accessed=count * 524_288, transcendentals=0
        ),
    )(me, w)


def join_kernel(where, me_ref, *refs):
    me = me_ref[0]
    out_ref = refs[-1]
    for i in range(out_ref.shape[0]):
        for ref, places in zip(refs, where):
            for place, r in places:
                at = pl.multiple_of(((me & 7) ^ r) * LANES, LANES)
                out_ref[i, :, pl.ds(at, LANES)] = ref[place, i]


def join(out, pieces, me, which, other, step, slot=0):
    first, count = which
    assert count % step == 0 and slot % step == 0
    base = slot // step
    in_specs, args, where = [], [], []
    for array, taken, rs in pieces:
        in_specs.append(pl.BlockSpec((taken, step, ROWS, LANES), lambda e, m: (0, base + e, 0, 0)))
        args.append(array)
        where.append([(i, r) for i, r in enumerate(rs)])
    alias = {}
    if out is not None:
        in_specs.append(pl.BlockSpec(memory_space=pl.ANY))
        args.append(out)
        alias = {len(args): 0}
    return pl.pallas_call(
        functools.partial(join_kernel, where),
        grid_spec=pltpu.PrefetchScalarGridSpec(
            num_scalar_prefetch=1,
            grid=(count // step,),
            in_specs=in_specs,
            out_specs=pl.BlockSpec(
                (pl.Element(step), pl.Element(ROWS), pl.Element(1024)),
                lambda e, m: (first + e * step, 0, ((m[0] >> 3) ^ other) * 1024),
            ),
        ),
        out_shape=jax.ShapeDtypeStruct((EXPERTS, ROWS, D_MODEL), jnp.bfloat16),
        input_output_aliases=alias,
        name="join",
        cost_estimate=pl.CostEstimate(
            flops=count * 1_000_000, bytes_accessed=count * 262_144, transcendentals=0
        ),
    )(me, *args)


def plane(arrays):
    have = [arrays[0]] + [swap(arrays[k], k) for k in (1, 2, 3)]
    return have, swap(pack([(a, 1, 2) for a in have]), 4)


def plane_y(arrays):
    kept, sent = arrays
    over_y = swap(sent, 4)
    pieces = [(kept, 1, [0]), (over_y, 1, [4])]
    for k in (1, 2, 3):
        both = pack([(kept, k, k + 1), (over_y, k, k + 1)])
        pieces.append((swap(both, k), 2, [k, 4 + k]))
    return pieces


def by_x(came):
    return [came[2 * k : 2 * k + 2] for k in range(4)]


def pieces_of(have, over_y):
    return [(have[k], 1, [k]) for k in range(4)] + [(over_y, 4, [4, 5, 6, 7])]


def router_kernel(where, me_ref, *refs):
    me = me_ref[0]
    for ref, places in zip(refs, where):
        for place, r in places:
            for z in range(2):
                at = pl.multiple_of((me ^ (8 * z + r)) * LANES, LANES)
                refs[-1][:, pl.ds(at, LANES)] = ref[place, z]


def router_join(pieces, me, slot):
    where = [list(enumerate(rs)) for _, _, rs in pieces]
    assert slot % 2 == 0
    return pl.pallas_call(
        functools.partial(router_kernel, where),
        grid_spec=pltpu.PrefetchScalarGridSpec(
            num_scalar_prefetch=1,
            grid=(1,),
            in_specs=[
                pl.BlockSpec((taken, 2, ROWS, LANES), lambda e, m: (0, slot // 2, 0, 0))
                for _, taken, _ in pieces
            ],
            out_specs=pl.BlockSpec((ROWS, D_MODEL), lambda e, m: (0, 0)),
        ),
        out_shape=jax.ShapeDtypeStruct((ROWS, D_MODEL), jnp.bfloat16),
        name="router",
        cost_estimate=pl.CostEstimate(flops=2_000_000, bytes_accessed=524_288, transcendentals=0),
    )(me, *[array for array, _, _ in pieces])


def on_device(w_down, router_weight, router_gain):
    index = lax.axis_index("fsdp").astype(jnp.int32)
    me = index.reshape(1)

    sums = jnp.sum(jnp.abs(w_down), axis=2).reshape(EXPERTS, 8, LANES)
    for k in (1, 2, 4, 8):
        sums = sums + swap(sums, k)

    part = (router_weight * router_gain[:, None]).astype(jnp.bfloat16).T
    part = lax.all_to_all(jnp.broadcast_to(part[None], (4, 16, LANES)), "ep", 0, 0, tiled=True)
    part = part.reshape(ROWS, LANES)
    router = (part, swap(part, 8))

    raws = spread_raw(w_down, me, E)
    raws = [swap(raw, 8) for raw in raws]

    (oth_f,) = spread(w_down, sums, me, F, 1, 1, 7)
    came_f = swap(oth_f, 8)
    oth_l = spread(w_down, sums, me, L, 1, 4, 7)
    own_b = spread_own(w_down, sums, router, raws, me, B)
    own_a = spread(w_down, sums, me, A, 0, 4, 5)

    plane_l = plane(oth_l)
    last = pack([(a, 0, 1) for a in plane_l[0]] + [(plane_l[1], 0, 4)])
    came_l = swap(last, 8)
    plane_b = plane_y(own_b)
    plane_a = plane(own_a)
    plane_f = plane(by_x(came_f))

    scale = lax.dynamic_slice_in_dim(sums.reshape(EXPERTS, 16, ROWS), index, 1, 1)[:, 0] / D_MODEL

    out = join(None, plane_b, me, B, 0, B[1])
    out = join(out, pieces_of(*plane_a), me, A, 0, 5)
    serve_router = router_join(plane_b, me, B[1]).T
    out = join(out, plane_b, me, E, 1, 2, B[1] + 2)
    out = join(out, pieces_of(*plane_f), me, F, 1, 7)
    out = join(out, [(came_l, 8, list(range(8)))], me, L, 1, 7)
    return (out, scale, serve_router)


def solution(mesh):
    return jax.shard_map(
        on_device,
        mesh=mesh,
        in_specs=(P(("unit", "ep"), None, "fsdp"), P(("unit", "fsdp"), "ep"), P(("unit", "fsdp"))),
        out_specs=(P(("unit", "ep"), "fsdp", None), P(("unit", "ep"), "fsdp"), P("unit", None)),
        check_vma=False,
    )
```

```python
import functools

import jax
import jax.numpy as jnp
from jax import lax
from jax.experimental import pallas as pl
from jax.experimental.pallas import tpu as pltpu
from jax.sharding import PartitionSpec as P

D_MODEL = 2048
EXPERTS = 16
ROWS = 64
LANES = 128
HALF = 512

F, L, E = (0, 7), (7, 7), (14, 2)
RAW = (1, 1)
A, B = (0, 10), (10, 6)


def swap(shard, k):
    return lax.ppermute(shard, "fsdp", [(i, i ^ k) for i in range(lax.axis_size("fsdp"))])


def pack(parts):
    return jnp.concatenate([array[first:end] for array, first, end in parts], 0)


def relative(s, m):
    s = jnp.where((m & 8) != 0, jnp.concatenate([s[4:8], s[0:4]], 0), s)
    s = jnp.where((m & 4) != 0, jnp.concatenate([s[2:4], s[0:2], s[6:8], s[4:6]], 0), s)
    odd = [s[i ^ 1 : (i ^ 1) + 1] for i in range(8)]
    s = jnp.where((m & 2) != 0, jnp.concatenate(odd, 0), s)
    return jnp.where((m & 1) != 0, jnp.concatenate([s[:, ROWS:], s[:, :ROWS]], 1), s)


def spread_kernel(other, scaled, me_ref, w_ref, *refs):
    m = me_ref[0] ^ (8 * other)
    outs = refs[1:] if scaled else refs
    for i in range(w_ref.shape[0]):
        if scaled:
            inverse = (D_MODEL / relative(refs[0][i], m)).T
        for r in range(8):
            at = pl.multiple_of(((m & 7) ^ r) * ROWS, ROWS)
            block = w_ref[i, pl.ds(at, ROWS), :]
            if scaled:
                h = (r & 1) * ROWS
                block = block * inverse[h : h + ROWS, r >> 1 : (r >> 1) + 1]
            y, x = r >> 2, r & 3
            if not scaled:
                outs[int(i >= RAW[0])][2 * x + y, i % RAW[0]] = block
            elif len(outs) == 4:
                outs[x][y, i] = block.astype(outs[x].dtype)
            elif len(outs) == 2:
                outs[y][x, i] = block.astype(outs[y].dtype)
            else:
                outs[0][2 * x + y, i] = block.astype(outs[0].dtype)


def spread(w, sums, me, which, other, arrays, step):
    first, count = which
    scaled = sums is not None
    kind = jnp.bfloat16 if scaled else jnp.float32
    assert count % step == 0
    blocks = 8 // arrays
    in_specs = [
        pl.BlockSpec(
            (pl.Element(step), pl.Element(HALF), pl.Element(LANES)),
            lambda e, m: (first + e * step, ((m[0] >> 3) ^ other) * HALF, 0),
        )
    ]
    args = [w]
    if scaled:
        in_specs.append(
            pl.BlockSpec(
                (pl.Element(step), pl.Element(8), pl.Element(LANES)),
                lambda e, m: (first + e * step, 0, 0),
            )
        )
        args.append(sums)
    return pl.pallas_call(
        functools.partial(spread_kernel, other, scaled),
        grid_spec=pltpu.PrefetchScalarGridSpec(
            num_scalar_prefetch=1,
            grid=(count // step,),
            in_specs=in_specs,
            out_specs=[pl.BlockSpec((blocks, step, ROWS, LANES), lambda e, m: (0, e, 0, 0))]
            * arrays,
        ),
        out_shape=[jax.ShapeDtypeStruct((blocks, count, ROWS, LANES), kind)] * arrays,
        name="spread",
        cost_estimate=pl.CostEstimate(
            flops=count * 1_000_000, bytes_accessed=count * 393_216, transcendentals=0
        ),
    )(me, *args)


def own_kernel(me_ref, w_ref, s_ref, near_ref, far_ref, *refs):
    m = me_ref[0]
    raws, outs = refs[:-2], refs[-2:]
    count = w_ref.shape[0]
    for i in range(count):
        inverse = (D_MODEL / relative(s_ref[i], m)).T
        for r in range(8):
            at = pl.multiple_of(((m & 7) ^ r) * ROWS, ROWS)
            column = inverse[(r & 1) * ROWS : (r & 1) * ROWS + ROWS, r >> 1 : (r >> 1) + 1]
            outs[r >> 2][r & 3, i] = (w_ref[i, pl.ds(at, ROWS), :] * column).astype(jnp.bfloat16)
            raw = i - (count - E[1])
            if raw >= 0:
                block = raws[int(raw >= RAW[0])][2 * (r & 3) + (r >> 2), raw % RAW[0]] * column
                outs[r >> 2][r & 3, count + 2 + raw] = block.astype(jnp.bfloat16)
    for out in outs:
        for x in range(4):
            out[x, count] = near_ref[...]
            out[x, count + 1] = far_ref[...]


def spread_own(w, sums, router, raws, me, which):
    first, count = which
    slots = count + 2 + E[1]

    def whole(*shape):
        return pl.BlockSpec(shape, lambda e, m: (0,) * len(shape))

    return pl.pallas_call(
        own_kernel,
        grid_spec=pltpu.PrefetchScalarGridSpec(
            num_scalar_prefetch=1,
            grid=(1,),
            in_specs=[
                pl.BlockSpec(
                    (pl.Element(count), pl.Element(HALF), pl.Element(LANES)),
                    lambda e, m: (first, (m[0] >> 3) * HALF, 0),
                ),
                pl.BlockSpec(
                    (pl.Element(count), pl.Element(8), pl.Element(LANES)),
                    lambda e, m: (first, 0, 0),
                ),
                whole(ROWS, LANES),
                whole(ROWS, LANES),
            ]
            + [whole(8, n, ROWS, LANES) for n in RAW],
            out_specs=[whole(4, slots, ROWS, LANES)] * 2,
        ),
        out_shape=[jax.ShapeDtypeStruct((4, slots, ROWS, LANES), jnp.bfloat16)] * 2,
        name="spread_own",
        cost_estimate=pl.CostEstimate(
            flops=slots * 1_000_000, bytes_accessed=slots * 393_216, transcendentals=0
        ),
    )(me, w, sums, *router, *raws)


def spread_raw(w, me, which):
    first, count = which
    return pl.pallas_call(
        functools.partial(spread_kernel, 1, False),
        grid_spec=pltpu.PrefetchScalarGridSpec(
            num_scalar_prefetch=1,
            grid=(1,),
            in_specs=[
                pl.BlockSpec(
                    (pl.Element(count), pl.Element(HALF), pl.Element(LANES)),
                    lambda e, m: (first, ((m[0] >> 3) ^ 1) * HALF, 0),
                )
            ],
            out_specs=[pl.BlockSpec((8, n, ROWS, LANES), lambda e, m: (0, 0, 0, 0)) for n in RAW],
        ),
        out_shape=[jax.ShapeDtypeStruct((8, n, ROWS, LANES), jnp.float32) for n in RAW],
        name="spread_raw",
        cost_estimate=pl.CostEstimate(
            flops=count * 1_000_000, bytes_accessed=count * 524_288, transcendentals=0
        ),
    )(me, w)


def join_kernel(where, me_ref, *refs):
    me = me_ref[0]
    out_ref = refs[-1]
    for i in range(out_ref.shape[0]):
        for ref, places in zip(refs, where):
            for place, r in places:
                at = pl.multiple_of(((me & 7) ^ r) * LANES, LANES)
                out_ref[i, :, pl.ds(at, LANES)] = ref[place, i]


def join(out, pieces, me, which, other, step, slot=0):
    first, count = which
    assert count % step == 0
    in_specs, args, where = [], [], []
    for array, taken, rs in pieces:
        shape = tuple(pl.Element(n) for n in (taken, step, ROWS, LANES))
        in_specs.append(pl.BlockSpec(shape, lambda e, m: (0, slot + e * step, 0, 0)))
        args.append(array)
        where.append([(i, r) for i, r in enumerate(rs)])
    alias = {}
    if out is not None:
        in_specs.append(pl.BlockSpec(memory_space=pl.ANY))
        args.append(out)
        alias = {len(args): 0}
    return pl.pallas_call(
        functools.partial(join_kernel, where),
        grid_spec=pltpu.PrefetchScalarGridSpec(
            num_scalar_prefetch=1,
            grid=(count // step,),
            in_specs=in_specs,
            out_specs=pl.BlockSpec(
                (pl.Element(step), pl.Element(ROWS), pl.Element(1024)),
                lambda e, m: (first + e * step, 0, ((m[0] >> 3) ^ other) * 1024),
            ),
        ),
        out_shape=jax.ShapeDtypeStruct((EXPERTS, ROWS, D_MODEL), jnp.bfloat16),
        input_output_aliases=alias,
        name="join",
        cost_estimate=pl.CostEstimate(
            flops=count * 1_000_000, bytes_accessed=count * 262_144, transcendentals=0
        ),
    )(me, *args)


def plane(arrays):
    have = [arrays[0]] + [swap(arrays[k], k) for k in (1, 2, 3)]
    return have, swap(pack([(a, 1, 2) for a in have]), 4)


def plane_y(arrays):
    kept, sent = arrays
    over_y = swap(sent, 4)
    pieces = [(kept, 1, [0]), (over_y, 1, [4])]
    for k in (1, 2, 3):
        both = pack([(kept, k, k + 1), (over_y, k, k + 1)])
        pieces.append((swap(both, k), 2, [k, 4 + k]))
    return pieces


def by_x(came):
    return [came[2 * k : 2 * k + 2] for k in range(4)]


def pieces_of(have, over_y):
    return [(have[k], 1, [k]) for k in range(4)] + [(over_y, 4, [4, 5, 6, 7])]


def router_kernel(where, me_ref, *refs):
    me = me_ref[0]
    for ref, places in zip(refs, where):
        for place, r in places:
            for z in range(2):
                at = pl.multiple_of((me ^ (8 * z + r)) * LANES, LANES)
                refs[-1][:, pl.ds(at, LANES)] = ref[place, z]


def router_join(pieces, me, slot):
    where = [list(enumerate(rs)) for _, _, rs in pieces]
    assert slot % 2 == 0
    return pl.pallas_call(
        functools.partial(router_kernel, where),
        grid_spec=pltpu.PrefetchScalarGridSpec(
            num_scalar_prefetch=1,
            grid=(1,),
            in_specs=[
                pl.BlockSpec((taken, 2, ROWS, LANES), lambda e, m: (0, slot // 2, 0, 0))
                for _, taken, _ in pieces
            ],
            out_specs=pl.BlockSpec((ROWS, D_MODEL), lambda e, m: (0, 0)),
        ),
        out_shape=jax.ShapeDtypeStruct((ROWS, D_MODEL), jnp.bfloat16),
        name="router",
        cost_estimate=pl.CostEstimate(flops=2_000_000, bytes_accessed=524_288, transcendentals=0),
    )(me, *[array for array, _, _ in pieces])


def on_device(w_down, router_weight, router_gain):
    index = lax.axis_index("fsdp").astype(jnp.int32)
    me = index.reshape(1)

    sums = jnp.sum(jnp.abs(w_down), axis=2).reshape(EXPERTS, 8, LANES)
    for k in (1, 2, 4, 8):
        sums = sums + swap(sums, k)

    part = (router_weight * router_gain[:, None]).astype(jnp.bfloat16).T
    part = lax.all_to_all(jnp.broadcast_to(part[None], (4, 16, LANES)), "ep", 0, 0, tiled=True)
    part = part.reshape(ROWS, LANES)
    router = (part, swap(part, 8))

    raws = spread_raw(w_down, me, E)
    raws = [swap(raw, 8) for raw in raws]

    (oth_f,) = spread(w_down, sums, me, F, 1, 1, F[1])
    came_f = swap(oth_f, 8)
    oth_l = spread(w_down, sums, me, L, 1, 4, L[1])
    own_b = spread_own(w_down, sums, router, raws, me, B)
    own_a = spread(w_down, sums, me, A, 0, 2, 5)

    plane_l = plane(oth_l)
    last = pack([(a, 0, 1) for a in plane_l[0]] + [(plane_l[1], 0, 4)])
    came_l = swap(last, 8)
    plane_b = plane_y(own_b)
    plane_a = plane_y(own_a)
    plane_f = plane(by_x(came_f))

    scale = lax.dynamic_slice_in_dim(sums.reshape(EXPERTS, 16, ROWS), index, 1, 1)[:, 0] / D_MODEL

    out = join(None, plane_b, me, B, 0, B[1])
    serve_router = router_join(plane_b, me, B[1]).T
    out = join(out, plane_b, me, E, 1, E[1], B[1] + 2)
    out = join(out, plane_a, me, A, 0, 5)
    out = join(out, pieces_of(*plane_f), me, F, 1, F[1])
    out = join(out, [(came_l, 8, list(range(8)))], me, L, 1, L[1])
    return (out, scale, serve_router)


def solution(mesh):
    return jax.shard_map(
        on_device,
        mesh=mesh,
        in_specs=(P(("unit", "ep"), None, "fsdp"), P(("unit", "fsdp"), "ep"), P(("unit", "fsdp"))),
        out_specs=(P(("unit", "ep"), "fsdp", None), P(("unit", "ep"), "fsdp"), P("unit", None)),
        check_vma=False,
    )
```

```python
import functools

import jax
import jax.numpy as jnp
from jax import lax
from jax.experimental import pallas as pl
from jax.experimental.pallas import tpu as pltpu
from jax.sharding import PartitionSpec as P

D_MODEL = 2048
EXPERTS = 16
ROWS = 64
LANES = 128
HALF = 512

F, L, E = (0, 6), (6, 7), (13, 3)
RAW = (2, 1)
A, B = (0, 10), (10, 6)

SMALL = pltpu.CompilerParams(vmem_limit_bytes=12 * 2**20)


def swap(shard, k):
    return lax.ppermute(shard, "fsdp", [(i, i ^ k) for i in range(lax.axis_size("fsdp"))])


def pack(parts):
    return jnp.concatenate([array[first:end] for array, first, end in parts], 0)


def relative(s, m):
    s = jnp.where((m & 8) != 0, jnp.concatenate([s[4:8], s[0:4]], 0), s)
    s = jnp.where((m & 4) != 0, jnp.concatenate([s[2:4], s[0:2], s[6:8], s[4:6]], 0), s)
    odd = [s[i ^ 1 : (i ^ 1) + 1] for i in range(8)]
    s = jnp.where((m & 2) != 0, jnp.concatenate(odd, 0), s)
    return jnp.where((m & 1) != 0, jnp.concatenate([s[:, ROWS:], s[:, :ROWS]], 1), s)


def spread_kernel(other, scaled, me_ref, w_ref, *refs):
    m = me_ref[0] ^ (8 * other)
    outs = refs[1:] if scaled else refs
    for i in range(w_ref.shape[0]):
        if scaled:
            inverse = (D_MODEL / relative(refs[0][i], m)).T
        for r in range(8):
            at = pl.multiple_of(((m & 7) ^ r) * ROWS, ROWS)
            block = w_ref[i, pl.ds(at, ROWS), :]
            if scaled:
                h = (r & 1) * ROWS
                block = block * inverse[h : h + ROWS, r >> 1 : (r >> 1) + 1]
            y, x = r >> 2, r & 3
            if not scaled:
                outs[int(i >= RAW[0])][2 * x + y, i % RAW[0]] = block
            elif len(outs) == 4:
                outs[x][y, i] = block.astype(outs[x].dtype)
            elif len(outs) == 2:
                outs[y][x, i] = block.astype(outs[y].dtype)
            else:
                outs[0][2 * x + y, i] = block.astype(outs[0].dtype)


def spread(w, sums, me, which, other, arrays, step):
    first, count = which
    scaled = sums is not None
    kind = jnp.bfloat16 if scaled else jnp.float32
    assert count % step == 0
    blocks = 8 // arrays
    in_specs = [
        pl.BlockSpec(
            (pl.Element(step), pl.Element(HALF), pl.Element(LANES)),
            lambda e, m: (first + e * step, ((m[0] >> 3) ^ other) * HALF, 0),
        )
    ]
    args = [w]
    if scaled:
        in_specs.append(
            pl.BlockSpec(
                (pl.Element(step), pl.Element(8), pl.Element(LANES)),
                lambda e, m: (first + e * step, 0, 0),
            )
        )
        args.append(sums)
    return pl.pallas_call(
        functools.partial(spread_kernel, other, scaled),
        grid_spec=pltpu.PrefetchScalarGridSpec(
            num_scalar_prefetch=1,
            grid=(count // step,),
            in_specs=in_specs,
            out_specs=[pl.BlockSpec((blocks, step, ROWS, LANES), lambda e, m: (0, e, 0, 0))]
            * arrays,
        ),
        out_shape=[jax.ShapeDtypeStruct((blocks, count, ROWS, LANES), kind)] * arrays,
        name="spread",
        compiler_params=SMALL,
        cost_estimate=pl.CostEstimate(
            flops=count * 1_000_000, bytes_accessed=count * 393_216, transcendentals=0
        ),
    )(me, *args)


def own_kernel(me_ref, w_ref, s_ref, near_ref, far_ref, *refs):
    m = me_ref[0]
    raws, outs = refs[:-2], refs[-2:]
    count = w_ref.shape[0]
    for i in range(count):
        inverse = (D_MODEL / relative(s_ref[i], m)).T
        for r in range(8):
            at = pl.multiple_of(((m & 7) ^ r) * ROWS, ROWS)
            column = inverse[(r & 1) * ROWS : (r & 1) * ROWS + ROWS, r >> 1 : (r >> 1) + 1]
            outs[r >> 2][r & 3, i] = (w_ref[i, pl.ds(at, ROWS), :] * column).astype(jnp.bfloat16)
            raw = i - (count - E[1])
            if raw >= 0:
                block = raws[int(raw >= RAW[0])][2 * (r & 3) + (r >> 2), raw % RAW[0]] * column
                outs[r >> 2][r & 3, count + 2 + raw] = block.astype(jnp.bfloat16)
    for out in outs:
        for x in range(4):
            out[x, count] = near_ref[...]
            out[x, count + 1] = far_ref[...]


def spread_own(w, sums, router, raws, me, which):
    first, count = which
    slots = count + 2 + E[1]

    def whole(*shape):
        return pl.BlockSpec(shape, lambda e, m: (0,) * len(shape))

    return pl.pallas_call(
        own_kernel,
        grid_spec=pltpu.PrefetchScalarGridSpec(
            num_scalar_prefetch=1,
            grid=(1,),
            in_specs=[
                pl.BlockSpec(
                    (pl.Element(count), pl.Element(HALF), pl.Element(LANES)),
                    lambda e, m: (first, (m[0] >> 3) * HALF, 0),
                ),
                pl.BlockSpec(
                    (pl.Element(count), pl.Element(8), pl.Element(LANES)),
                    lambda e, m: (first, 0, 0),
                ),
                whole(ROWS, LANES),
                whole(ROWS, LANES),
            ]
            + [whole(8, n, ROWS, LANES) for n in RAW],
            out_specs=[whole(4, slots, ROWS, LANES)] * 2,
        ),
        out_shape=[jax.ShapeDtypeStruct((4, slots, ROWS, LANES), jnp.bfloat16)] * 2,
        name="spread_own",
        compiler_params=SMALL,
        cost_estimate=pl.CostEstimate(
            flops=slots * 1_000_000, bytes_accessed=slots * 393_216, transcendentals=0
        ),
    )(me, w, sums, *router, *raws)


def spread_raw(w, me, which):
    first, count = which
    return pl.pallas_call(
        functools.partial(spread_kernel, 1, False),
        grid_spec=pltpu.PrefetchScalarGridSpec(
            num_scalar_prefetch=1,
            grid=(1,),
            in_specs=[
                pl.BlockSpec(
                    (pl.Element(count), pl.Element(HALF), pl.Element(LANES)),
                    lambda e, m: (first, ((m[0] >> 3) ^ 1) * HALF, 0),
                )
            ],
            out_specs=[pl.BlockSpec((8, n, ROWS, LANES), lambda e, m: (0, 0, 0, 0)) for n in RAW],
        ),
        out_shape=[jax.ShapeDtypeStruct((8, n, ROWS, LANES), jnp.float32) for n in RAW],
        name="spread_raw",
        cost_estimate=pl.CostEstimate(
            flops=count * 1_000_000, bytes_accessed=count * 524_288, transcendentals=0
        ),
    )(me, w)


def join_kernel(where, me_ref, *refs):
    me = me_ref[0]
    out_ref = refs[-1]
    for i in range(out_ref.shape[0]):
        for ref, places in zip(refs, where):
            for place, r in places:
                at = pl.multiple_of(((me & 7) ^ r) * LANES, LANES)
                out_ref[i, :, pl.ds(at, LANES)] = ref[place, i]


def join(out, pieces, me, which, other, step, slot=0):
    first, count = which
    assert count % step == 0
    in_specs, args, where = [], [], []
    for array, taken, rs in pieces:
        shape = tuple(pl.Element(n) for n in (taken, step, ROWS, LANES))
        in_specs.append(pl.BlockSpec(shape, lambda e, m: (0, slot + e * step, 0, 0)))
        args.append(array)
        where.append([(i, r) for i, r in enumerate(rs)])
    alias = {}
    if out is not None:
        in_specs.append(pl.BlockSpec(memory_space=pl.ANY))
        args.append(out)
        alias = {len(args): 0}
    return pl.pallas_call(
        functools.partial(join_kernel, where),
        grid_spec=pltpu.PrefetchScalarGridSpec(
            num_scalar_prefetch=1,
            grid=(count // step,),
            in_specs=in_specs,
            out_specs=pl.BlockSpec(
                (pl.Element(step), pl.Element(ROWS), pl.Element(1024)),
                lambda e, m: (first + e * step, 0, ((m[0] >> 3) ^ other) * 1024),
            ),
        ),
        out_shape=jax.ShapeDtypeStruct((EXPERTS, ROWS, D_MODEL), jnp.bfloat16),
        input_output_aliases=alias,
        name="join",
        compiler_params=SMALL,
        cost_estimate=pl.CostEstimate(
            flops=count * 1_000_000, bytes_accessed=count * 262_144, transcendentals=0
        ),
    )(me, *args)


def plane(arrays):
    have = [arrays[0]] + [swap(arrays[k], k) for k in (1, 2, 3)]
    return have, swap(pack([(a, 1, 2) for a in have]), 4)


def plane_y(arrays):
    kept, sent = arrays
    over_y = swap(sent, 4)
    pieces = [(kept, 1, [0]), (over_y, 1, [4])]
    for k in (1, 2, 3):
        both = pack([(kept, k, k + 1), (over_y, k, k + 1)])
        pieces.append((swap(both, k), 2, [k, 4 + k]))
    return pieces


def by_x(came):
    return [came[2 * k : 2 * k + 2] for k in range(4)]


def pieces_of(have, over_y):
    return [(have[k], 1, [k]) for k in range(4)] + [(over_y, 4, [4, 5, 6, 7])]


def join_b_kernel(where, me_ref, *refs):
    me = me_ref[0]
    out_ref, router_ref = refs[-2:]
    count = out_ref.shape[0]
    for ref, places in zip(refs, where):
        for place, r in places:
            near = pl.ds(pl.multiple_of((me ^ r) * LANES, LANES), LANES)
            far = pl.ds(pl.multiple_of((me ^ r ^ 8) * LANES, LANES), LANES)
            for i in range(count):
                out_ref[i, :, near] = ref[place, i]
            router_ref[:, near] = ref[place, count]
            router_ref[:, far] = ref[place, count + 1]
            for i in range(E[1]):
                out_ref[count - E[1] + i, :, far] = ref[place, count + 2 + i]


def join_b(out, pieces, me):
    first, count = B
    assert first + count == E[0] + E[1] == EXPERTS and E[0] >= first
    slots = count + 2 + E[1]
    where = [list(enumerate(rs)) for _, _, rs in pieces]
    return pl.pallas_call(
        functools.partial(join_b_kernel, where),
        grid_spec=pltpu.PrefetchScalarGridSpec(
            num_scalar_prefetch=1,
            grid=(1,),
            in_specs=[
                pl.BlockSpec((taken, slots, ROWS, LANES), lambda e, m: (0, 0, 0, 0))
                for _, taken, _ in pieces
            ]
            + [pl.BlockSpec(memory_space=pl.ANY)],
            out_specs=[
                pl.BlockSpec(
                    (pl.Element(count), pl.Element(ROWS), pl.Element(D_MODEL)),
                    lambda e, m: (first, 0, 0),
                ),
                pl.BlockSpec((ROWS, D_MODEL), lambda e, m: (0, 0)),
            ],
        ),
        out_shape=[
            jax.ShapeDtypeStruct((EXPERTS, ROWS, D_MODEL), jnp.bfloat16),
            jax.ShapeDtypeStruct((ROWS, D_MODEL), jnp.bfloat16),
        ],
        input_output_aliases={len(pieces) + 1: 0},
        name="join_b",
        compiler_params=SMALL,
        cost_estimate=pl.CostEstimate(flops=8_000_000, bytes_accessed=2_097_152, transcendentals=0),
    )(me, *[array for array, _, _ in pieces], out)


def on_device(w_down, router_weight, router_gain):
    index = lax.axis_index("fsdp").astype(jnp.int32)
    me = index.reshape(1)

    sums = jnp.sum(jnp.abs(w_down), axis=2).reshape(EXPERTS, 8, LANES)
    for k in (1, 2, 4, 8):
        sums = sums + swap(sums, k)

    part = (router_weight * router_gain[:, None]).astype(jnp.bfloat16).T
    part = lax.all_to_all(jnp.broadcast_to(part[None], (4, 16, LANES)), "ep", 0, 0, tiled=True)
    part = part.reshape(ROWS, LANES)
    router = (part, swap(part, 8))

    raws = spread_raw(w_down, me, E)
    raws = [swap(raw, 8) for raw in raws]

    (oth_f,) = spread(w_down, sums, me, F, 1, 1, F[1])
    came_f = swap(oth_f, 8)
    oth_l = spread(w_down, sums, me, L, 1, 4, L[1])
    own_b = spread_own(w_down, sums, router, raws, me, B)
    own_a = spread(w_down, sums, me, A, 0, 2, 5)

    plane_l = plane(oth_l)
    last = pack([(a, 0, 1) for a in plane_l[0]] + [(plane_l[1], 0, 4)])
    came_l = swap(last, 8)
    plane_b = plane_y(own_b)
    plane_a = plane_y(own_a)
    plane_f = plane(by_x(came_f))

    scale = lax.dynamic_slice_in_dim(sums.reshape(EXPERTS, 16, ROWS), index, 1, 1)[:, 0] / D_MODEL

    out = join(None, plane_a, me, A, 0, 5)
    out, router = join_b(out, plane_b, me)
    out = join(out, pieces_of(*plane_f), me, F, 1, F[1])
    out = join(out, [(came_l, 8, list(range(8)))], me, L, 1, L[1])
    return (out, scale, router.T)


def solution(mesh):
    return jax.shard_map(
        on_device,
        mesh=mesh,
        in_specs=(P(("unit", "ep"), None, "fsdp"), P(("unit", "fsdp"), "ep"), P(("unit", "fsdp"))),
        out_specs=(P(("unit", "ep"), "fsdp", None), P(("unit", "ep"), "fsdp"), P("unit", None)),
        check_vma=False,
    )
```
